32 devices in a mesh: rows: 8 (over z, x), cols: 4 (over y, core).
Axes of the slice: x: 2, y: 2, z: 4, core: 2. Of those that a mesh axis runs over, the one named last changes fastest.
Arguments:
- basis: float32 [65536, 256], P(('rows', 'cols')), may hold values from -8 to 8, as said below
- new_vectors: float32 [65536, 128], P(('rows', 'cols')), may hold values from -180 to 180
- jacobian: float32 [65536, 1024], P(('rows', 'cols')), may hold values from -0.1875 to 0.1875
Outputs:
- merged: float32 [65536, 384], P(('rows', 'cols'))
The draws below stay inside these ranges and needn't reach their ends.
Inputs may be any that keep to these rules, and one draw needn't show every extreme that they name: The stored basis is orthonormal under the inner product divided by 65536 up to a drift of orthogonality: basis^T basis / 65536 differs from the identity by about 0.1 to 0.3 in spectral norm.
All inputs are finite; a program needn't handle non-finite values.
Results may differ from the reference program's by a relative error of at most 0.00005.
Values sent between devices are 32-bit elements; how exact they have to be, the bound alone decides.
No kernel may reach another device: no remote copies, remote signals or barrier semaphores. Data moves between devices by JAX's collectives and lax.ppermute only.
A program may use at most 64 MiB of HBM per device.

```python
import math
import jax
import jax.numpy as jnp
from jax import lax

K = 256
B = 128
OBS = 1024
NT = 65536


def draw_basis(key, part):
    raw_key = jax.random.fold_in(key, 5)
    drift_key = jax.random.fold_in(key, 7)
    raw = jax.random.normal(raw_key, (NT, K), jnp.float32)
    gram = lax.dot_general(raw, raw, (((0,), (0,)), ((), ())), precision=lax.Precision.HIGHEST, preferred_element_type=jnp.float32) / NT
    lower = jnp.linalg.cholesky(gram)
    ident = jnp.eye(K, dtype=jnp.float32)
    inverse = lax.linalg.triangular_solve(lower, ident, left_side=True, lower=True)
    ortho = jnp.dot(raw, inverse.T, precision=lax.Precision.HIGHEST, preferred_element_type=jnp.float32)
    drift = jax.random.normal(drift_key, (K, K), jnp.float32) * (0.05 / math.sqrt(K))
    mixed = jnp.dot(ortho, ident + drift, precision=lax.Precision.HIGHEST, preferred_element_type=jnp.float32)
    return jnp.clip(mixed, -8.0, 8.0)


def draw_new_vectors(key, part):
    first_key = jax.random.fold_in(key, 11)
    second_key = jax.random.fold_in(key, 23)
    positions = jnp.arange(NT, dtype=jnp.float32)
    factor = 1.0 + 2.0 * positions / max(NT - 1, 1)
    base = jax.random.normal(first_key, (NT, B), jnp.float32)
    scales = jnp.exp(jax.random.uniform(second_key, (1, B), jnp.float32, 0.0, math.log(10.0)))
    return jnp.clip(base * scales * factor[:, None], -180.0, 180.0)


def block_levels(key, shape, pieces, low, top_value):
    def one(position, shards_of):
        heights = jax.random.uniform(jax.random.fold_in(jax.random.fold_in(key, 6), position), (shards_of,), jnp.float32, low / len(pieces), top_value / len(pieces))
        return jnp.repeat(jnp.exp(heights), shape[position] // shards_of).reshape((-1,) + (1,) * (len(shape) - position - 1))

    factor_of = one(*pieces[0])
    for cut in pieces[1:]:
        factor_of = factor_of * one(*cut)
    return factor_of


def centred(rng, shape, width, limit, shards=(), kind=jnp.bfloat16):
    entries = width * jax.random.normal(rng, shape, jnp.float32)
    if shards:
        entries = entries * block_levels(rng, shape, shards, -0.22, 0.18)
    return jnp.clip(entries, -limit, limit).astype(kind)


def setup_inputs(seed: int = 0) -> dict:
    keys = jax.random.split(jax.random.key(seed), 4)
    basis = draw_basis(jax.random.fold_in(keys[3], 71), 0)
    new_vectors = draw_new_vectors(jax.random.fold_in(keys[3], 71), 0)
    jacobian = centred(keys[2], (NT, OBS), OBS ** -0.5, 0.1875, ((0, 32),), jnp.float32)
    return {"basis": basis, "new_vectors": new_vectors, "jacobian": jacobian}


def mat(left, right):
    return jnp.dot(left.astype(jnp.float32), right.astype(jnp.float32), precision=lax.Precision.HIGHEST, preferred_element_type=jnp.float32)

def tmat(left, right):
    return lax.dot_general(left.astype(jnp.float32), right.astype(jnp.float32), (((0,), (0,)), ((), ())), precision=lax.Precision.HIGHEST, preferred_element_type=jnp.float32)

def inverse_lower(gram):
    lower = jnp.linalg.cholesky(gram)
    ident = jnp.eye(gram.shape[0], dtype=jnp.float32)
    return lax.linalg.triangular_solve(lower, ident, left_side=True, lower=True)

def reference(basis, new_vectors, jacobian):
    scale = 1.0 / NT
    root = 1.0 / jnp.sqrt(jnp.float32(NT))
    first = tmat(basis, new_vectors) * scale
    once = new_vectors - mat(basis, first)
    second = tmat(basis, once) * scale
    cleaned = once - mat(basis, second)
    gram = tmat(cleaned, cleaned) * scale
    fresh = mat(cleaned, inverse_lower(gram).T)
    joined = jnp.concatenate([basis, fresh], axis=1)
    proj = tmat(jacobian, joined) * root
    hess = tmat(proj, proj)
    ident = jnp.eye(hess.shape[0], dtype=jnp.float32)
    outer = inverse_lower(ident + hess)
    return mat(joined, outer.T)
```

```python
import jax
import jax.numpy as jnp
from jax import lax
from jax.experimental import pallas as pl
from jax.experimental.pallas import tpu as pltpu
from jax.sharding import PartitionSpec as P

F32 = jnp.float32
BF16 = jnp.bfloat16
LANES = 128
BLOCK = 16
VMEM = pltpu.MemorySpace.VMEM


def halves(value):
    high = value.astype(BF16)
    return high, (value - high.astype(F32)).astype(BF16)


def thirds(value):
    high = value.astype(BF16)
    rest = value - high.astype(F32)
    middle = rest.astype(BF16)
    return high, middle, (rest - middle.astype(F32)).astype(BF16)


def contract(left, right, left_dim, right_dim):
    return lax.dot_general(
        left, right, (((left_dim,), (right_dim,)), ((), ())), preferred_element_type=F32
    )


def three(left, right, left_dim, right_dim):
    return (
        contract(left[0], right[0], left_dim, right_dim)
        + contract(left[0], right[1], left_dim, right_dim)
        + contract(left[1], right[0], left_dim, right_dim)
    )


def exact(left, right, left_dim, right_dim):
    return lax.dot_general(
        left,
        right,
        (((left_dim,), (right_dim,)), ((), ())),
        precision=lax.Precision.HIGHEST,
        preferred_element_type=F32,
    )


def products_kernel(which_ref, basis_ref, new_ref, jac_ref, out_ref):
    step = pl.program_id(0)

    @pl.when(step == 0)
    def _():
        out_ref[...] = jnp.zeros_like(out_ref)

    shards = out_ref.shape[0]
    wide = basis_ref.shape[1] + new_ref.shape[1]
    lane = jac_ref.shape[1] // shards
    stacked = halves(jnp.concatenate([basis_ref[...], new_ref[...]], axis=1))
    jac = halves(jac_ref[...])
    prod = three(stacked, jac, 0, 0)
    for s in range(shards):
        out_ref[s, :wide, :] += prod[:, s * lane : (s + 1) * lane]
    tiles = wide // LANES
    pairs = [(i, j) for i in range(tiles) for j in range(i, tiles)]
    half = len(pairs) // 2
    piece = out_ref.shape[1] - wide

    def tile(index):
        return tuple(part[:, index * LANES : (index + 1) * LANES] for part in stacked)

    def gram(which):
        def run():
            blocks = [three(tile(i), tile(j), 0, 0) for i, j in pairs[which * half : (which + 1) * half]]
            rows = jnp.concatenate(blocks, axis=0)
            for s in range(shards):
                out_ref[s, wide:, :] += rows[s * piece : (s + 1) * piece]

        return run

    pl.when(which_ref[0] == 0)(gram(0))
    pl.when(which_ref[0] == 1)(gram(1))


def products(which, basis, new_vectors, jacobian):
    rows, width = basis.shape
    block = new_vectors.shape[1]
    wide = width + block
    obs = jacobian.shape[1]
    tiles = wide // LANES
    packed = tiles * (tiles + 1) // 2 * LANES
    chunk = rows // 4
    return pl.pallas_call(
        products_kernel,
        grid_spec=pltpu.PrefetchScalarGridSpec(
            num_scalar_prefetch=1,
            grid=(rows // chunk,),
            in_specs=[
                pl.BlockSpec((chunk, width), lambda k, w: (k, 0)),
                pl.BlockSpec((chunk, block), lambda k, w: (k, 0)),
                pl.BlockSpec((chunk, obs // 2), lambda k, w: (k, w[0])),
            ],
            out_specs=pl.BlockSpec((4, wide + packed // 8, obs // 8), lambda k, w: (0, 0, 0)),
        ),
        out_shape=jax.ShapeDtypeStruct((4, wide + packed // 8, obs // 8), F32),
    )(which, basis, new_vectors, jacobian)


def factor(m_ref):
    n = m_ref.shape[0]
    tiles = n // LANES
    for phase in range(tiles):
        base = LANES * phase

        def step(k, carry, base=base):
            start = base + k * BLOCK
            mine = pl.ds(pl.multiple_of(start, BLOCK), BLOCK)
            rows = m_ref[mine, :]
            diag = rows[:, base : base + LANES]
            row = lax.broadcasted_iota(jnp.int32, (BLOCK, LANES), 0)
            cols = [
                jnp.take_along_axis(diag, jnp.full((BLOCK, LANES), k * BLOCK + q, jnp.int32), axis=1)
                for q in range(BLOCK)
            ]
            lane = lax.broadcasted_iota(jnp.int32, (BLOCK, n), 1) - start
            sub = lax.broadcasted_iota(jnp.int32, (BLOCK, n), 0)
            unit = jnp.where(lane == sub, 1.0, 0.0)
            work = jnp.where((lane >= 0) & (lane < BLOCK), unit, rows)
            parts = [work[:, t * LANES : (t + 1) * LANES] for t in range(tiles)]
            pivots = jnp.ones((BLOCK, LANES), F32)
            for p in range(BLOCK):
                pivot = jnp.broadcast_to(cols[p][p : p + 1, :], (BLOCK, LANES))
                pivots = jnp.where(row == p, pivot, pivots)
                if p + 1 < BLOCK:
                    mult = jnp.where(row > p, cols[p], 0.0) * (1.0 / pivot)
                    for q in range(p + 1, BLOCK):
                        cols[q] = cols[q] - mult * jnp.broadcast_to(cols[q][p : p + 1, :], (BLOCK, LANES))
                    parts = [x - mult * jnp.broadcast_to(x[p : p + 1, :], (BLOCK, LANES)) for x in parts]
            inv = lax.rsqrt(pivots)
            done = jnp.concatenate([x * inv for x in parts], axis=1)
            rest = jnp.where(lane >= BLOCK, done, 0.0)[:, base:]
            h, m, l = thirds(done)
            hr, mr, lr = thirds(rest)
            right = jnp.concatenate([h, m, h, l, h, m, l, m], axis=0)
            left = jnp.concatenate([hr, hr, mr, hr, lr, mr, mr, lr], axis=0)
            update = contract(left, right, 0, 0)
            lanes = lax.broadcasted_iota(jnp.int32, (n - base, n), 1) - start
            keep = (lanes < 0) | (lanes >= BLOCK)
            m_ref[base:, :] = jnp.where(keep, m_ref[base:, :], 0.0) - update
            m_ref[mine, :] = done
            return carry

        lax.fori_loop(0, LANES // BLOCK, step, 0)


def whiten_kernel(width, scale, gram_ref, hess_ref, out_ref):
    n = out_ref.shape[0]
    tiles = n // LANES
    pairs = [(i, j) for i in range(tiles) for j in range(i, tiles)]

    def whole(ref):
        blocks = {}
        for index, (i, j) in enumerate(pairs):
            value = ref[index * LANES : (index + 1) * LANES, :] * scale
            blocks[i, j] = value
            if i != j:
                blocks[j, i] = value.T
        return jnp.concatenate(
            [jnp.concatenate([blocks[i, j] for j in range(tiles)], axis=1) for i in range(tiles)], axis=0
        )

    full = whole(gram_ref)
    hess = whole(hess_ref)
    s_vv, s_vw, s_ww = full[:width, :width], full[:width, width:], full[width:, width:]
    second = s_vw - exact(s_vv, s_vw, 1, 0)
    summed = s_vw + second
    gram = s_ww - exact(summed, s_vw, 0, 0) - exact(s_vw, summed, 0, 0)
    gram = gram + exact(summed, exact(s_vv, summed, 1, 0), 0, 0)
    corner = exact(summed, summed, 0, 0) + gram
    r = lax.broadcasted_iota(jnp.int32, (width, width), 0)
    c = lax.broadcasted_iota(jnp.int32, (width, width), 1)
    out_ref[:width, :width] = hess[:width, :width] + jnp.where(r == c, 1.0, 0.0)
    out_ref[:width, width:] = hess[:width, width:] + summed
    out_ref[width:, :width] = hess[width:, :width] + summed.T
    out_ref[width:, width:] = hess[width:, width:] + corner
    factor(out_ref)
    r = lax.broadcasted_iota(jnp.int32, (n, n), 0)
    c = lax.broadcasted_iota(jnp.int32, (n, n), 1)
    out_ref[...] = jnp.where(r >= c, out_ref[...], 0.0)


def whiten(width, n, scale, gram, hess):
    def kernel(gram_ref, hess_ref, out_ref):
        whiten_kernel(width, scale, gram_ref, hess_ref, out_ref)

    return pl.pallas_call(
        kernel,
        in_specs=[pl.BlockSpec(memory_space=VMEM)] * 2,
        out_specs=pl.BlockSpec(memory_space=VMEM),
        out_shape=jax.ShapeDtypeStruct((n, n), F32),
    )(gram, hess)


def apply_kernel(basis_ref, new_ref, inv_ref, out_ref):
    width = basis_ref.shape[1]
    old = halves(basis_ref[...])
    new = halves(new_ref[...])
    inv = halves(inv_ref[...])
    top = tuple(x[:width, :width] for x in inv)
    left = tuple(x[width:, :width] for x in inv)
    corner = tuple(x[width:, width:] for x in inv)
    out_ref[:, :width] = three(old, top, 1, 1)
    out_ref[:, width:] = three(old, left, 1, 1) + three(new, corner, 1, 1)


def apply(basis, new_vectors, inv):
    rows, width = basis.shape
    block = new_vectors.shape[1]
    wide = width + block
    chunk = rows // 4
    return pl.pallas_call(
        apply_kernel,
        grid=(rows // chunk,),
        in_specs=[
            pl.BlockSpec((chunk, width), lambda k: (k, 0)),
            pl.BlockSpec((chunk, block), lambda k: (k, 0)),
            pl.BlockSpec((wide, wide), lambda k: (0, 0)),
        ],
        out_specs=pl.BlockSpec((chunk, wide), lambda k: (k, 0)),
        out_shape=jax.ShapeDtypeStruct((rows, wide), F32),
    )(basis, new_vectors, inv)


def swap(value, axis, mask):
    size = lax.axis_size(axis)
    return lax.ppermute(value, axis, [(i, i ^ mask) for i in range(size)])


def pick(value, index, dim):
    return lax.dynamic_index_in_dim(value, index, dim, keepdims=False)


def ordered(bit, own, other):
    return jnp.stack([jnp.where(bit == 0, own, other), jnp.where(bit == 0, other, own)])


def local(basis, new_vectors, jacobian):
    n_rows, n_cols = lax.axis_size("rows"), lax.axis_size("cols")
    total = basis.shape[0] * n_rows * n_cols
    width = basis.shape[1]
    wide = width + new_vectors.shape[1]
    at_row, at_col = lax.axis_index("rows"), lax.axis_index("cols")
    c, y, x = at_col & 1, (at_col >> 1) & 1, at_row & 1
    rest = [("cols", 1 << b) for b in range(2, n_cols.bit_length() - 1)]
    rest += [("rows", m) for m in (2, 6) if m < n_rows]
    rest += [("rows", 1 << b) for b in range(3, n_rows.bit_length() - 1)]

    theirs = products((1 - c).reshape(1), basis, new_vectors, jacobian)
    got = swap(theirs, "cols", 1)
    mine = products(c.reshape(1), basis, new_vectors, jacobian)
    both = (mine + got).reshape(2, 2, *mine.shape[1:])
    cut = both.shape[2] // 2
    a, b = both[:, :, :cut], both[:, :, cut:]
    got_a = swap(pick(a, 1 - y, 0), "cols", 2)
    got_b = swap(pick(b, 1 - x, 1), "rows", 1)
    a = pick(a, y, 0) + got_a
    b = pick(b, x, 1) + got_b
    got_a = swap(pick(a, 1 - x, 0), "rows", 1)
    got_b = swap(pick(b, 1 - y, 0), "cols", 2)
    a = pick(a, x, 0) + got_a
    b = pick(b, y, 0) + got_b
    for (axis_a, mask_a), (axis_b, mask_b) in zip(rest, rest[::-1]):
        got_a = swap(a, axis_a, mask_a)
        got_b = swap(b, axis_b, mask_b)
        a, b = a + got_a, b + got_b
    shard = jnp.concatenate([a, b], axis=0)
    proj, gram = shard[:wide], shard[wide:]

    tiles = wide // LANES
    hess = exact(proj, proj, 1, 1)
    hess = jnp.concatenate(
        [
            hess[i * LANES : (i + 1) * LANES, j * LANES : (j + 1) * LANES]
            for i in range(tiles)
            for j in range(i, tiles)
        ],
        axis=0,
    ).reshape(2, -1, LANES)
    hess = pick(hess, c, 0) + swap(pick(hess, 1 - c, 0), "cols", 1)
    cut = hess.shape[0] // 2
    h_a, h_b = hess[:cut], hess[cut:]
    g_cut = gram.shape[0] // 2
    g_a, g_b = gram[:g_cut], gram[g_cut:]
    got_a = swap(jnp.concatenate([h_a, g_a]), "cols", 2)
    got_b = swap(jnp.concatenate([h_b, g_b]), "rows", 1)
    h_a, h_b = h_a + got_a[:cut], h_b + got_b[:cut]
    g_a = ordered(y, g_a, got_a[cut:])
    g_b = ordered(x, g_b, got_b[cut:])
    got_a = swap(jnp.concatenate([h_a, g_a.reshape(-1, LANES)]), "rows", 1)
    got_b = swap(jnp.concatenate([h_b, g_b.reshape(-1, LANES)]), "cols", 2)
    h_a, h_b = h_a + got_a[:cut], h_b + got_b[:cut]
    g_a = ordered(x, g_a, got_a[cut:].reshape(g_a.shape))
    g_b = ordered(y, g_b, got_b[cut:].reshape(g_b.shape))
    gram = jnp.concatenate([jnp.swapaxes(g_a, 0, 1), g_b], axis=2).reshape(-1, LANES)
    hess = jnp.concatenate([h_a, h_b])
    send = jnp.stack([hess, gram])
    full = ordered(c, send, swap(send, "cols", 1))
    hess = full[:, 0].reshape(-1, LANES)
    gram = full[:, 1].reshape(-1, LANES)
    inv = whiten(width, wide, 1.0 / total, gram, hess)
    return apply(basis, new_vectors, inv)


def solution(mesh):
    placed = (P(("rows", "cols"), None), P(("rows", "cols"), None), P(("rows", "cols"), None))
    return jax.shard_map(
        local, mesh=mesh, in_specs=placed, out_specs=P(("rows", "cols"), None), check_vma=False
    )
```

```python
import functools

import jax
import jax.numpy as jnp
from jax import lax
from jax.experimental import pallas as pl
from jax.experimental.pallas import tpu as pltpu
from jax.sharding import PartitionSpec as P

F32 = jnp.float32
BF16 = jnp.bfloat16
LANES = 128
BLOCK = 16
CHUNKS = 4
LIMIT = pltpu.CompilerParams(vmem_limit_bytes=32 << 20)
VMEM = pltpu.VMEM


def halves(value):
    high = value.astype(BF16)
    return high, (value - high.astype(F32)).astype(BF16)


def thirds(value):
    high = value.astype(BF16)
    rest = value - high.astype(F32)
    middle = rest.astype(BF16)
    return high, middle, (rest - middle.astype(F32)).astype(BF16)


def contract(left, right, left_dim, right_dim):
    return lax.dot_general(
        left, right, (((left_dim,), (right_dim,)), ((), ())), preferred_element_type=F32
    )


def three(left, right, left_dim, right_dim):
    return (
        contract(left[0], right[0], left_dim, right_dim)
        + contract(left[0], right[1], left_dim, right_dim)
        + contract(left[1], right[0], left_dim, right_dim)
    )


def exact(left, right, left_dim, right_dim):
    return lax.dot_general(
        left,
        right,
        (((left_dim,), (right_dim,)), ((), ())),
        precision=lax.Precision.HIGHEST,
        preferred_element_type=F32,
    )


def spread(outs, value, extra):
    lanes = outs[0].shape[2]
    piece = extra.shape[0] // outs[0].shape[0]
    cut = outs[0].shape[1]
    tall = value.shape[0]
    for s in range(outs[0].shape[0]):
        tile = value[:, s * lanes : (s + 1) * lanes]
        outs[0][s, :, :] = tile[:cut]
        outs[1][s, : tall - cut, :] = tile[cut:]
        outs[1][s, tall - cut :, :] = extra[s * piece : (s + 1) * piece]


def products_kernel(first, core_ref, basis_ref, new_ref, jac_ref, *refs):
    if first:
        out_a_ref, out_b_ref, own_ref, vec_ref, obs_ref, sems = refs
    else:
        own_ref, out_a_ref, out_b_ref, vec_ref, obs_ref, sems = refs
    rows, width = basis_ref.shape
    wide = vec_ref.shape[1]
    part = obs_ref.shape[1]
    chunk = rows // CHUNKS
    index = 1 - core_ref[0] if first else core_ref[0]
    lanes = pl.ds(pl.multiple_of(index * part, part), part)

    def copies(k):
        at = pl.ds(k * chunk, chunk)
        return (
            pltpu.make_async_copy(basis_ref.at[at, :], vec_ref.at[at, pl.ds(0, width)], sems.at[k, 0]),
            pltpu.make_async_copy(new_ref.at[at, :], vec_ref.at[at, pl.ds(width, wide - width)], sems.at[k, 1]),
            pltpu.make_async_copy(jac_ref.at[at, lanes], obs_ref.at[at, :], sems.at[k, 2]),
        )

    for k in range(CHUNKS):
        for copy in copies(k):
            copy.start()
    total = None
    for k in range(CHUNKS):
        for copy in copies(k):
            copy.wait()
        at = slice(k * chunk, (k + 1) * chunk)
        value = vec_ref[at, :]
        flipped = halves(value.T)
        sums = [three(flipped, halves(obs_ref[at, :]), 1, 0)]
        if first:
            stacked = halves(value)
            sums += [contract(flipped[0], part, 1, 0) for part in stacked]
        total = sums if total is None else [x + y for x, y in zip(total, sums)]
    if not first:
        spread((out_a_ref, out_b_ref), total[0], own_ref[...])
        return
    prod, near, far = total
    gram = near + far + far.T
    tiles = wide // LANES
    blocks = [gram[i * LANES : (i + 1) * LANES, j * LANES : (j + 1) * LANES] for j in range(tiles) for i in range(j, tiles)]
    half = len(blocks) // 2
    low, high = (jnp.concatenate(blocks[k * half : (k + 1) * half], axis=0) for k in range(2))
    lead = core_ref[0] == 1
    spread((out_a_ref, out_b_ref), prod, jnp.where(lead, low, high))
    own_ref[...] = jnp.where(lead, high, low)


def products(core, basis, new_vectors, jacobian):
    rows, width = basis.shape
    wide = width + new_vectors.shape[1]
    obs = jacobian.shape[1]
    tiles = wide // LANES
    packed = tiles * (tiles + 1) // 2 * LANES // 8
    sums = VMEM((4, (wide + packed) // 2, obs // 8), F32)
    own = VMEM((4 * packed, obs // 8), F32)
    inside = pl.BlockSpec(memory_space=VMEM)
    outside = pl.BlockSpec(memory_space=pltpu.HBM)
    scalar = pl.BlockSpec(memory_space=pltpu.SMEM)

    def call(first, *more):
        return pl.pallas_call(
            functools.partial(products_kernel, first),
            in_specs=[scalar, outside, outside, outside] + [inside] * len(more),
            out_specs=[inside] * (3 if first else 2),
            out_shape=[sums, sums, own] if first else [sums, sums],
            scratch_shapes=[
                VMEM((rows, wide), F32),
                VMEM((rows, obs // 2), F32),
                pltpu.SemaphoreType.DMA((CHUNKS, 3)),
            ],
            compiler_params=LIMIT,
        )(core, basis, new_vectors, jacobian, *more)

    *theirs, own = call(True)
    return call(False, own), theirs


def factor(m_ref):
    n = m_ref.shape[0]
    tiles = n // LANES
    for phase in range(tiles):
        base = LANES * phase

        def step(k, carry, base=base):
            start = base + k * BLOCK
            mine = pl.ds(pl.multiple_of(start, BLOCK), BLOCK)
            rows = m_ref[mine, :]
            diag = rows[:, base : base + LANES]
            row = lax.broadcasted_iota(jnp.int32, (BLOCK, LANES), 0)
            cols = [
                jnp.take_along_axis(diag, jnp.full((BLOCK, LANES), k * BLOCK + q, jnp.int32), axis=1)
                for q in range(BLOCK)
            ]
            lane = lax.broadcasted_iota(jnp.int32, (BLOCK, n), 1) - start
            sub = lax.broadcasted_iota(jnp.int32, (BLOCK, n), 0)
            unit = jnp.where(lane == sub, 1.0, 0.0)
            work = jnp.where((lane >= 0) & (lane < BLOCK), unit, rows)
            parts = [work[:, t * LANES : (t + 1) * LANES] for t in range(tiles)]
            pivots = jnp.ones((BLOCK, LANES), F32)
            for p in range(0, BLOCK, 2):
                base_row = (p + 1) // 8 * 8

                def wide_row(value, index, low=base_row):
                    return jnp.broadcast_to(value[index : index + 1, :], (BLOCK - low, LANES))

                a, b, c = wide_row(cols[p], p, 0), wide_row(cols[p], p + 1, 0), wide_row(cols[p + 1], p + 1, 0)
                det = a * c - b * b
                over_det, over_a = 1.0 / det, 1.0 / a
                pivots = jnp.where(row == p, a, jnp.where(row == p + 1, det * over_a, pivots))
                under = row[base_row:] > p + 1
                x, y = cols[p][base_row:], cols[p + 1][base_row:]
                a, b, c, ratio, over_det = (v[base_row:] for v in (a, b, c, b * over_a, over_det))
                mult = jnp.where(under, (x * c - y * b) * over_det, 0.0)
                next_mult = jnp.where(under, (y * a - x * b) * over_det, 0.0)

                def cleared(value, first_mult, p=p, low=base_row, next_mult=next_mult, wide_row=wide_row):
                    new = value[low:] - first_mult * wide_row(value, p) - next_mult * wide_row(value, p + 1)
                    return jnp.concatenate([value[:low], new], axis=0) if low else new

                for q in range(p + 2, BLOCK):
                    cols[q] = cleared(cols[q], mult)
                mult = jnp.where(row[base_row:] == p + 1, ratio, mult)
                parts = [cleared(value, mult) for value in parts]
            inv = lax.rsqrt(pivots)
            done = jnp.concatenate([x * inv for x in parts], axis=1)
            rest = jnp.where(lane >= BLOCK, done, 0.0)[:, base:]
            h, m, l = thirds(done)
            hr, mr, lr = thirds(rest)
            right = jnp.concatenate([h, m, h, l, h, m, l, m], axis=0)
            left = jnp.concatenate([hr, hr, mr, hr, lr, mr, mr, lr], axis=0)
            update = contract(left, right, 0, 0)
            lanes = lax.broadcasted_iota(jnp.int32, (n - base, n), 1) - start
            keep = (lanes < 0) | (lanes >= BLOCK)
            m_ref[base:, :] = jnp.where(keep, m_ref[base:, :], 0.0) - update
            m_ref[mine, :] = done
            return carry

        lax.fori_loop(0, LANES // BLOCK, step, 0)


def hess_kernel(core_ref, a_ref, got_a_ref, b_ref, got_b_ref, keep_a_ref, keep_b_ref, give_a_ref, give_b_ref, gram_a_ref, gram_b_ref):
    shard = jnp.concatenate([a_ref[...] + got_a_ref[...], b_ref[...] + got_b_ref[...]], axis=0)
    cut = gram_a_ref.shape[0]
    wide = shard.shape[0] - 2 * cut
    tiles = wide // LANES
    hess = exact(shard[:wide], shard[:wide], 1, 1)
    blocks = [
        hess[i * LANES : (i + 1) * LANES, j * LANES : (j + 1) * LANES] for j in range(tiles) for i in range(j, tiles)
    ]
    half = len(blocks) // 2
    first, second = (jnp.concatenate(blocks[k * half : (k + 1) * half], axis=0) for k in range(2))
    lead = core_ref[0] == 1
    keep, give = jnp.where(lead, second, first), jnp.where(lead, first, second)
    middle = keep_a_ref.shape[0]
    keep_a_ref[...], keep_b_ref[...] = keep[:middle], keep[middle:]
    give_a_ref[...], give_b_ref[...] = give[:middle], give[middle:]
    gram_a_ref[...], gram_b_ref[...] = shard[wide : wide + cut], shard[wide + cut :]


def shard_hess(core, wide, a, got_a, b, got_b):
    inside = pl.BlockSpec(memory_space=VMEM)
    tiles = wide // LANES
    part = VMEM((tiles * (tiles + 1) * LANES // 8, LANES), F32)
    gram = VMEM(((2 * a.shape[0] - wide) // 2, LANES), F32)
    return pl.pallas_call(
        hess_kernel,
        in_specs=[pl.BlockSpec(memory_space=pltpu.SMEM)] + [inside] * 4,
        out_specs=[inside] * 6,
        out_shape=[part] * 4 + [gram] * 2,
        compiler_params=LIMIT,
    )(core, a, got_a, b, got_b)


def whiten_kernel(scale, lead_ref, own_ref, got_ref, basis_ref, new_ref, out_ref, m_ref, vec_ref, res_ref, sems):
    n = m_ref.shape[0]
    rows, width = basis_ref.shape
    chunk = rows // CHUNKS

    def loads(k):
        at = pl.ds(k * chunk, chunk)
        return (
            pltpu.make_async_copy(basis_ref.at[at, :], vec_ref.at[at, pl.ds(0, width)], sems.at[k, 0]),
            pltpu.make_async_copy(new_ref.at[at, :], vec_ref.at[at, pl.ds(width, n - width)], sems.at[k, 1]),
        )

    for k in range(CHUNKS):
        for copy in loads(k):
            copy.start()
    tiles = n // LANES
    pairs = [(i, j) for j in range(tiles) for i in range(j, tiles)]
    half = len(pairs) // 2
    lead = lead_ref[0] == 1

    def whole(which):
        blocks = {}
        for index, (i, j) in enumerate(pairs):
            rest = index % half * LANES
            at = slice(rest, rest + LANES)
            value = jnp.where(lead == (index >= half), own_ref[which, at, :], got_ref[which, at, :]) * scale
            blocks[i, j] = value
            if i != j:
                blocks[j, i] = value.T
        return jnp.concatenate(
            [jnp.concatenate([blocks[i, j] for j in range(tiles)], axis=1) for i in range(tiles)], axis=0
        )

    hess = whole(0)
    full = whole(1)
    s_vv, s_vw, s_ww = full[:width, :width], full[:width, width:], full[width:, width:]
    second = s_vw - exact(s_vv, s_vw, 1, 0)
    summed = s_vw + second
    gram = s_ww - exact(summed, s_vw, 0, 0) - exact(s_vw, summed, 0, 0)
    gram = gram + exact(summed, exact(s_vv, summed, 1, 0), 0, 0)
    corner = exact(summed, summed, 0, 0) + gram
    r = lax.broadcasted_iota(jnp.int32, (width, width), 0)
    c = lax.broadcasted_iota(jnp.int32, (width, width), 1)
    m_ref[:width, :width] = hess[:width, :width] + jnp.where(r == c, 1.0, 0.0)
    m_ref[:width, width:] = hess[:width, width:] + summed
    m_ref[width:, :width] = hess[width:, :width] + summed.T
    m_ref[width:, width:] = hess[width:, width:] + corner
    factor(m_ref)
    r = lax.broadcasted_iota(jnp.int32, (n, n), 0)
    c = lax.broadcasted_iota(jnp.int32, (n, n), 1)
    mix = halves(jnp.where(r >= c, m_ref[...], 0.0).T)
    corner = tuple(x[:width, :width] for x in mix)
    last = tuple(x[:, width:] for x in mix)

    def store(k):
        at = pl.ds(k * chunk, chunk)
        return pltpu.make_async_copy(res_ref.at[at, :], out_ref.at[at, :], sems.at[k, 2])

    for k in range(CHUNKS):
        at = slice(k * chunk, (k + 1) * chunk)
        for copy in loads(k):
            copy.wait()
        value = halves(vec_ref[at, :])
        old = tuple(x[:, :width] for x in value)
        res_ref[at, :width] = three(old, corner, 1, 0)
        res_ref[at, width:] = three(value, last, 1, 0)
        store(k).start()
    for k in range(CHUNKS):
        store(k).wait()


def whiten(scale, lead, own, got, basis, new_vectors):
    rows, width = basis.shape
    n = width + new_vectors.shape[1]

    def kernel(*refs):
        whiten_kernel(scale, *refs)

    inside = pl.BlockSpec(memory_space=VMEM)
    outside = pl.BlockSpec(memory_space=pltpu.HBM)
    return pl.pallas_call(
        kernel,
        in_specs=[pl.BlockSpec(memory_space=pltpu.SMEM), inside, inside, outside, outside],
        out_specs=outside,
        out_shape=jax.ShapeDtypeStruct((rows, n), F32),
        scratch_shapes=[
            VMEM((n, n), F32),
            VMEM((rows, n), F32),
            VMEM((rows, n), F32),
            pltpu.SemaphoreType.DMA((CHUNKS, 3)),
        ],
        compiler_params=LIMIT,
    )(lead, own, got, basis, new_vectors)


def pick(value, index):
    return lax.dynamic_index_in_dim(value, index, 0, keepdims=False)


def ordered(bit, own, other):
    return jnp.stack([jnp.where(bit == 0, own, other), jnp.where(bit == 0, other, own)])


def swap(value, axis, mask):
    size = lax.axis_size(axis)
    return lax.ppermute(value, axis, [(i, i ^ mask) for i in range(size)])


def local(basis, new_vectors, jacobian):
    n_rows, n_cols = lax.axis_size("rows"), lax.axis_size("cols")
    total = basis.shape[0] * n_rows * n_cols
    wide = basis.shape[1] + new_vectors.shape[1]
    at_row, at_col = lax.axis_index("rows"), lax.axis_index("cols")
    core, y, x = (at_col & 1).reshape(1), (at_col >> 1) & 1, at_row & 1
    rest = [("cols", 1 << b) for b in range(2, n_cols.bit_length() - 1)]
    rest += [("rows", m) for m in (2, 6) if m < n_rows]
    rest += [("rows", 1 << b) for b in range(3, n_rows.bit_length() - 1)]

    basis, new_vectors, jacobian = (
        pltpu.with_memory_space_constraint(value, pltpu.HBM) for value in (basis, new_vectors, jacobian)
    )
    mine, theirs = products(core, basis, new_vectors, jacobian)
    a, b = (value.reshape(2, 2, *value.shape[1:]) for value in mine)
    up_a, up_b = (swap(value, "cols", 1).reshape(a.shape) for value in theirs)

    def across(value, index):
        return lax.dynamic_index_in_dim(value, index, 1, keepdims=False)

    def both(value, up, got, at_y, at_x, index):
        return pick(pick(value, at_y), at_x) + pick(pick(up, at_y), at_x) + pick(got, index)

    got_a = swap(pick(a, 1 - y) + pick(up_a, 1 - y), "cols", 2)
    got_b = swap(across(b, 1 - x) + across(up_b, 1 - x), "rows", 1)
    next_a = swap(both(a, up_a, got_a, y, 1 - x, 1 - x), "rows", 1)
    next_b = swap(both(b, up_b, got_b, 1 - y, x, 1 - y), "cols", 2)
    a, got_a = both(a, up_a, got_a, y, x, x), next_a
    b, got_b = both(b, up_b, got_b, y, x, y), next_b
    for (axis_a, mask_a), (axis_b, mask_b) in zip(rest, rest[::-1]):
        a, b = a + got_a, b + got_b
        got_a = swap(a, axis_a, mask_a)
        got_b = swap(b, axis_b, mask_b)

    keep_a, keep_b, give_a, give_b, g_a, g_b = shard_hess(core, wide, a, got_a, b, got_b)
    h_a, h_b = keep_a + swap(give_a, "cols", 1), keep_b + swap(give_b, "cols", 1)
    cut = h_a.shape[0]
    got_a = swap(jnp.concatenate([h_a, g_a]), "cols", 2)
    got_b = swap(jnp.concatenate([h_b, g_b]), "rows", 1)
    h_a, h_b = h_a + got_a[:cut], h_b + got_b[:cut]
    g_a = ordered(y, g_a, got_a[cut:])
    g_b = ordered(x, g_b, got_b[cut:])
    got_a = swap(jnp.concatenate([h_a, g_a.reshape(-1, LANES)]), "rows", 1)
    got_b = swap(jnp.concatenate([h_b, g_b.reshape(-1, LANES)]), "cols", 2)
    h_a, h_b = h_a + got_a[:cut], h_b + got_b[:cut]
    g_a = ordered(x, g_a, got_a[cut:].reshape(g_a.shape))
    g_b = ordered(y, g_b, got_b[cut:].reshape(g_b.shape))
    gram = jnp.concatenate([jnp.swapaxes(g_a, 0, 1), g_b], axis=2).reshape(-1, LANES)
    own = jnp.stack([jnp.concatenate([h_a, h_b]), gram])
    return whiten(1.0 / total, core, own, swap(own, "cols", 1), basis, new_vectors)


def solution(mesh):
    placed = (P(("rows", "cols"), None), P(("rows", "cols"), None), P(("rows", "cols"), None))
    return jax.shard_map(
        local, mesh=mesh, in_specs=placed, out_specs=P(("rows", "cols"), None), check_vma=False
    )
```

```python
import functools

import jax
import jax.numpy as jnp
from jax import lax
from jax.experimental import pallas as pl
from jax.experimental.pallas import tpu as pltpu
from jax.sharding import PartitionSpec as P

F32 = jnp.float32
BF16 = jnp.bfloat16
LANES = 128
BLOCK = 16
PANEL = 2
CHUNKS = 4
LIMIT = pltpu.CompilerParams(vmem_limit_bytes=32 << 20)
VMEM = pltpu.VMEM


def halves(value):
    high = value.astype(BF16)
    return high, (value - high.astype(F32)).astype(BF16)


def thirds(value):
    high = value.astype(BF16)
    rest = value - high.astype(F32)
    middle = rest.astype(BF16)
    return high, middle, (rest - middle.astype(F32)).astype(BF16)


def contract(left, right, left_dim, right_dim):
    return lax.dot_general(
        left, right, (((left_dim,), (right_dim,)), ((), ())), preferred_element_type=F32
    )


def three(left, right, left_dim, right_dim):
    return (
        contract(left[0], right[0], left_dim, right_dim)
        + contract(left[0], right[1], left_dim, right_dim)
        + contract(left[1], right[0], left_dim, right_dim)
    )


def exact(left, right, left_dim, right_dim):
    return lax.dot_general(
        left,
        right,
        (((left_dim,), (right_dim,)), ((), ())),
        precision=lax.Precision.HIGHEST,
        preferred_element_type=F32,
    )


def spread(outs, value, extra):
    lanes = outs[0].shape[2]
    piece = extra.shape[0] // outs[0].shape[0]
    cut = outs[0].shape[1]
    tall = value.shape[0]
    for s in range(outs[0].shape[0]):
        tile = value[:, s * lanes : (s + 1) * lanes]
        outs[0][s, :, :] = tile[:cut]
        outs[1][s, : tall - cut, :] = tile[cut:]
        outs[1][s, tall - cut :, :] = extra[s * piece : (s + 1) * piece]


def products_kernel(first, core_ref, basis_ref, new_ref, jac_ref, *refs):
    if first:
        out_a_ref, out_b_ref, own_ref, vec_ref, obs_ref, sems = refs
    else:
        own_ref, out_a_ref, out_b_ref, vec_ref, obs_ref, sems = refs
    rows, width = basis_ref.shape
    wide = vec_ref.shape[1]
    part = obs_ref.shape[1]
    chunk = rows // CHUNKS
    index = 1 - core_ref[0] if first else core_ref[0]
    lanes = pl.ds(pl.multiple_of(index * part, part), part)

    def copies(k):
        at = pl.ds(k * chunk, chunk)
        return (
            pltpu.make_async_copy(basis_ref.at[at, :], vec_ref.at[at, pl.ds(0, width)], sems.at[k, 0]),
            pltpu.make_async_copy(new_ref.at[at, :], vec_ref.at[at, pl.ds(width, wide - width)], sems.at[k, 1]),
            pltpu.make_async_copy(jac_ref.at[at, lanes], obs_ref.at[at, :], sems.at[k, 2]),
        )

    for k in range(CHUNKS):
        for copy in copies(k):
            copy.start()
    total = None
    for k in range(CHUNKS):
        for copy in copies(k):
            copy.wait()
        at = slice(k * chunk, (k + 1) * chunk)
        value = vec_ref[at, :]
        flipped = halves(value.T)
        sums = [three(flipped, halves(obs_ref[at, :]), 1, 0)]
        if first:
            stacked = halves(value)
            sums += [contract(flipped[0], part, 1, 0) for part in stacked]
        total = sums if total is None else [x + y for x, y in zip(total, sums)]
    if not first:
        spread((out_a_ref, out_b_ref), total[0], own_ref[...])
        return
    prod, near, far = total
    gram = near + far + far.T
    tiles = wide // LANES
    blocks = [gram[i * LANES : (i + 1) * LANES, j * LANES : (j + 1) * LANES] for j in range(tiles) for i in range(j, tiles)]
    half = len(blocks) // 2
    low, high = (jnp.concatenate(blocks[k * half : (k + 1) * half], axis=0) for k in range(2))
    lead = core_ref[0] == 1
    spread((out_a_ref, out_b_ref), prod, jnp.where(lead, low, high))
    own_ref[...] = jnp.where(lead, high, low)


def products(core, basis, new_vectors, jacobian):
    rows, width = basis.shape
    wide = width + new_vectors.shape[1]
    obs = jacobian.shape[1]
    tiles = wide // LANES
    packed = tiles * (tiles + 1) // 2 * LANES // 8
    sums = VMEM((4, (wide + packed) // 2, obs // 8), F32)
    own = VMEM((4 * packed, obs // 8), F32)
    inside = pl.BlockSpec(memory_space=VMEM)
    outside = pl.BlockSpec(memory_space=pltpu.HBM)
    scalar = pl.BlockSpec(memory_space=pltpu.SMEM)

    def call(first, *more):
        return pl.pallas_call(
            functools.partial(products_kernel, first),
            in_specs=[scalar, outside, outside, outside] + [inside] * len(more),
            out_specs=[inside] * (3 if first else 2),
            out_shape=[sums, sums, own] if first else [sums, sums],
            scratch_shapes=[
                VMEM((rows, wide), F32),
                VMEM((rows, obs // 2), F32),
                pltpu.SemaphoreType.DMA((CHUNKS, 3)),
            ],
            compiler_params=LIMIT,
        )(core, basis, new_vectors, jacobian, *more)

    *theirs, own = call(True)
    return call(False, own), theirs


def eliminate(parts, tile, first):
    height = parts[0].shape[0]
    row = lax.broadcasted_iota(jnp.int32, (height, LANES), 0)
    lane = lax.broadcasted_iota(jnp.int32, (height, LANES), 1) - first
    cols = [
        jnp.take_along_axis(parts[tile], jnp.full((height, LANES), first + q, jnp.int32), axis=1) for q in range(BLOCK)
    ]
    parts = list(parts)
    parts[tile] = jnp.where((lane >= 0) & (lane < BLOCK), jnp.where(lane == row, 1.0, 0.0), parts[tile])
    head = row[:BLOCK]
    pivots = jnp.ones((BLOCK, LANES), F32)

    def spot(value, index, tall):
        return jnp.broadcast_to(value[index : index + 1, :], (tall, LANES))

    for p in range(0, BLOCK, 2):
        low = (p + 1) // 8 * 8
        a, b, c = spot(cols[p], p, height), spot(cols[p], p + 1, height), spot(cols[p + 1], p + 1, height)
        det = a * c - b * b
        over_det, over_a = 1.0 / det, 1.0 / a
        pivots = jnp.where(head == p, a[:BLOCK], jnp.where(head == p + 1, (det * over_a)[:BLOCK], pivots))
        under = row[low:] > p + 1
        x, y = cols[p][low:], cols[p + 1][low:]
        a, b, c, ratio, over_det = (v[low:] for v in (a, b, c, b * over_a, over_det))
        mult = jnp.where(under, (x * c - y * b) * over_det, 0.0)
        next_mult = jnp.where(under, (y * a - x * b) * over_det, 0.0)

        def cleared(value, first_mult, p=p, low=low, next_mult=next_mult):
            tall = height - low
            new = value[low:] - first_mult * spot(value, p, tall) - next_mult * spot(value, p + 1, tall)
            return jnp.concatenate([value[:low], new], axis=0) if low else new

        for q in range(p + 2, BLOCK):
            cols[q] = cleared(cols[q], mult)
        mult = jnp.where(row[low:] == p + 1, ratio, mult)
        parts = [cleared(value, mult) for value in parts]
    inv = lax.rsqrt(pivots)
    return [value[:BLOCK] * inv for value in parts], [value[BLOCK:] for value in parts]


def factor(m_ref, ready, beside):
    n = m_ref.shape[0]
    tiles = n // LANES
    panel = BLOCK * PANEL
    for phase in range(tiles):
        base = LANES * phase
        last = phase == tiles - 1
        if last:
            ready()

        def step(k, carry, base=base, phase=phase, last=last):
            start = base + k * panel
            if last:
                beside(k)
            mine = pl.ds(pl.multiple_of(start, panel), panel)
            rows = m_ref[mine, :]
            parts = [rows[:, t * LANES : (t + 1) * LANES] for t in range(tiles)]
            blocks = []
            for b in range(PANEL):
                top, parts = eliminate(parts, phase, k * panel + b * BLOCK)
                blocks.append(jnp.concatenate(top, axis=1))
            done = jnp.concatenate(blocks, axis=0)
            lane = lax.broadcasted_iota(jnp.int32, (panel, n), 1) - start
            sub = lax.broadcasted_iota(jnp.int32, (panel, n), 0)
            rest = jnp.where(lane >= panel, done, 0.0)[:, base:]
            done = jnp.where((lane < panel) & (lane > sub), 0.0, done)
            h, m, l = thirds(done)
            hr, mr, lr = thirds(rest)
            right = jnp.concatenate([h, m, h, l, h, m], axis=0)
            left = jnp.concatenate([hr, hr, mr, hr, lr, mr], axis=0)
            update = contract(left, right, 0, 0)
            lanes = lax.broadcasted_iota(jnp.int32, (n - base, n), 1) - start
            keep = (lanes < 0) | (lanes >= panel)
            m_ref[base:, :] = jnp.where(keep, m_ref[base:, :], 0.0) - update
            m_ref[mine, :] = done
            return carry

        lax.fori_loop(0, LANES // panel, step, 0)


def hess_kernel(core_ref, a_ref, got_a_ref, b_ref, got_b_ref, keep_a_ref, keep_b_ref, give_a_ref, give_b_ref, gram_a_ref, gram_b_ref):
    shard = jnp.concatenate([a_ref[...] + got_a_ref[...], b_ref[...] + got_b_ref[...]], axis=0)
    cut = gram_a_ref.shape[0]
    wide = shard.shape[0] - 2 * cut
    tiles = wide // LANES
    hess = exact(shard[:wide], shard[:wide], 1, 1)
    blocks = [
        hess[i * LANES : (i + 1) * LANES, j * LANES : (j + 1) * LANES] for j in range(tiles) for i in range(j, tiles)
    ]
    half = len(blocks) // 2
    first, second = (jnp.concatenate(blocks[k * half : (k + 1) * half], axis=0) for k in range(2))
    lead = core_ref[0] == 1
    keep, give = jnp.where(lead, second, first), jnp.where(lead, first, second)
    middle = keep_a_ref.shape[0]
    keep_a_ref[...], keep_b_ref[...] = keep[:middle], keep[middle:]
    give_a_ref[...], give_b_ref[...] = give[:middle], give[middle:]
    gram_a_ref[...], gram_b_ref[...] = shard[wide : wide + cut], shard[wide + cut :]


def shard_hess(core, wide, a, got_a, b, got_b):
    inside = pl.BlockSpec(memory_space=VMEM)
    tiles = wide // LANES
    part = VMEM((tiles * (tiles + 1) * LANES // 8, LANES), F32)
    gram = VMEM(((2 * a.shape[0] - wide) // 2, LANES), F32)
    return pl.pallas_call(
        hess_kernel,
        in_specs=[pl.BlockSpec(memory_space=pltpu.SMEM)] + [inside] * 4,
        out_specs=[inside] * 6,
        out_shape=[part] * 4 + [gram] * 2,
        compiler_params=LIMIT,
    )(core, a, got_a, b, got_b)


def whiten_kernel(scale, lead_ref, own_ref, got_ref, basis_ref, new_ref, out_ref, m_ref, vec_ref, res_ref, mix_ref, sems):
    n = m_ref.shape[0]
    rows, width = basis_ref.shape
    chunk = rows // CHUNKS

    def loads(k):
        at = pl.ds(k * chunk, chunk)
        return (
            pltpu.make_async_copy(basis_ref.at[at, :], vec_ref.at[at, pl.ds(0, width)], sems.at[k, 0]),
            pltpu.make_async_copy(new_ref.at[at, :], vec_ref.at[at, pl.ds(width, n - width)], sems.at[k, 1]),
        )

    for k in range(CHUNKS):
        for copy in loads(k):
            copy.start()
    tiles = n // LANES
    pairs = [(i, j) for j in range(tiles) for i in range(j, tiles)]
    half = len(pairs) // 2
    lead = lead_ref[0] == 1

    def whole(which):
        blocks = {}
        for index, (i, j) in enumerate(pairs):
            rest = index % half * LANES
            at = slice(rest, rest + LANES)
            value = jnp.where(lead == (index >= half), own_ref[which, at, :], got_ref[which, at, :]) * scale
            blocks[i, j] = value
            if i != j:
                blocks[j, i] = value.T
        return jnp.concatenate(
            [jnp.concatenate([blocks[i, j] for j in range(tiles)], axis=1) for i in range(tiles)], axis=0
        )

    hess = whole(0)
    full = whole(1)
    s_vv, s_vw, s_ww = full[:width, :width], full[:width, width:], full[width:, width:]
    second = s_vw - exact(s_vv, s_vw, 1, 0)
    summed = s_vw + second
    moved = second + exact(s_vv, summed, 1, 0)
    corner = s_ww + exact(
        jnp.concatenate([summed, s_vw], axis=0), jnp.concatenate([moved, -summed], axis=0), 0, 0
    )
    r = lax.broadcasted_iota(jnp.int32, (width, width), 0)
    c = lax.broadcasted_iota(jnp.int32, (width, width), 1)
    m_ref[:width, :width] = hess[:width, :width] + jnp.where(r == c, 1.0, 0.0)
    m_ref[:width, width:] = hess[:width, width:] + summed
    m_ref[width:, :width] = hess[width:, :width] + summed.T
    m_ref[width:, width:] = hess[width:, width:] + corner
    lead_cols = n - LANES

    def store(k, late):
        at = pl.ds(pl.multiple_of(k * chunk, chunk), chunk)
        lanes = pl.ds(lead_cols, LANES) if late else pl.ds(0, lead_cols)
        return pltpu.make_async_copy(res_ref.at[at, lanes], out_ref.at[at, lanes], sems.at[k, 2 + late])

    def triangle(low, high):
        r = lax.broadcasted_iota(jnp.int32, (high - low, high), 0) + low
        c = lax.broadcasted_iota(jnp.int32, (high - low, high), 1)
        return halves(jnp.where(r >= c, m_ref[low:high, :high], 0.0).T)

    def ready():
        mix_ref[0], mix_ref[1] = triangle(0, lead_cols)
        for k in range(CHUNKS):
            for copy in loads(k):
                copy.wait()

    def beside(k):
        at = pl.ds(pl.multiple_of(k * chunk, chunk), chunk)
        res_ref[at, :lead_cols] = three(halves(vec_ref[at, :lead_cols]), (mix_ref[0], mix_ref[1]), 1, 0)
        store(k, 0).start()

    factor(m_ref, ready, beside)
    last = triangle(lead_cols, n)
    for k in range(CHUNKS):
        at = slice(k * chunk, (k + 1) * chunk)
        res_ref[at, lead_cols:] = three(halves(vec_ref[at, :]), last, 1, 0)
        store(k, 1).start()
    for k in range(CHUNKS):
        store(k, 0).wait()
        store(k, 1).wait()


def whiten(scale, lead, own, got, basis, new_vectors):
    rows, width = basis.shape
    n = width + new_vectors.shape[1]

    def kernel(*refs):
        whiten_kernel(scale, *refs)

    inside = pl.BlockSpec(memory_space=VMEM)
    outside = pl.BlockSpec(memory_space=pltpu.HBM)
    return pl.pallas_call(
        kernel,
        in_specs=[pl.BlockSpec(memory_space=pltpu.SMEM), inside, inside, outside, outside],
        out_specs=outside,
        out_shape=jax.ShapeDtypeStruct((rows, n), F32),
        scratch_shapes=[
            VMEM((n, n), F32),
            VMEM((rows, n), F32),
            VMEM((rows, n), F32),
            VMEM((2, n - LANES, n - LANES), BF16),
            pltpu.SemaphoreType.DMA((CHUNKS, 4)),
        ],
        compiler_params=LIMIT,
    )(lead, own, got, basis, new_vectors)


def pick(value, index):
    return lax.dynamic_index_in_dim(value, index, 0, keepdims=False)


def ordered(bit, own, other):
    return jnp.stack([jnp.where(bit == 0, own, other), jnp.where(bit == 0, other, own)])


def swap(value, axis, mask):
    size = lax.axis_size(axis)
    return lax.ppermute(value, axis, [(i, i ^ mask) for i in range(size)])


def local(basis, new_vectors, jacobian):
    n_rows, n_cols = lax.axis_size("rows"), lax.axis_size("cols")
    total = basis.shape[0] * n_rows * n_cols
    wide = basis.shape[1] + new_vectors.shape[1]
    at_row, at_col = lax.axis_index("rows"), lax.axis_index("cols")
    core, y, x = (at_col & 1).reshape(1), (at_col >> 1) & 1, at_row & 1
    rest = [("cols", 1 << b) for b in range(2, n_cols.bit_length() - 1)]
    rest += [("rows", m) for m in (2, 6) if m < n_rows]
    rest += [("rows", 1 << b) for b in range(3, n_rows.bit_length() - 1)]

    basis, new_vectors, jacobian = (
        pltpu.with_memory_space_constraint(value, pltpu.HBM) for value in (basis, new_vectors, jacobian)
    )
    mine, theirs = products(core, basis, new_vectors, jacobian)
    a, b = (value.reshape(2, 2, *value.shape[1:]) for value in mine)
    up_a, up_b = (swap(value, "cols", 1).reshape(a.shape) for value in theirs)

    def across(value, index):
        return lax.dynamic_index_in_dim(value, index, 1, keepdims=False)

    def both(value, up, got, at_y, at_x, index):
        return pick(pick(value, at_y), at_x) + pick(pick(up, at_y), at_x) + pick(got, index)

    got_a = swap(pick(a, 1 - y) + pick(up_a, 1 - y), "cols", 2)
    got_b = swap(across(b, 1 - x) + across(up_b, 1 - x), "rows", 1)
    next_a = swap(both(a, up_a, got_a, y, 1 - x, 1 - x), "rows", 1)
    next_b = swap(both(b, up_b, got_b, 1 - y, x, 1 - y), "cols", 2)
    a, got_a = both(a, up_a, got_a, y, x, x), next_a
    b, got_b = both(b, up_b, got_b, y, x, y), next_b
    for (axis_a, mask_a), (axis_b, mask_b) in zip(rest, rest[::-1]):
        a, b = a + got_a, b + got_b
        got_a = swap(a, axis_a, mask_a)
        got_b = swap(b, axis_b, mask_b)

    keep_a, keep_b, give_a, give_b, g_a, g_b = shard_hess(core, wide, a, got_a, b, got_b)
    h_a, h_b = keep_a + swap(give_a, "cols", 1), keep_b + swap(give_b, "cols", 1)
    cut = h_a.shape[0]
    got_a = swap(jnp.concatenate([h_a, g_a]), "cols", 2)
    got_b = swap(jnp.concatenate([h_b, g_b]), "rows", 1)
    h_a, h_b = h_a + got_a[:cut], h_b + got_b[:cut]
    g_a = ordered(y, g_a, got_a[cut:])
    g_b = ordered(x, g_b, got_b[cut:])
    got_a = swap(jnp.concatenate([h_a, g_a.reshape(-1, LANES)]), "rows", 1)
    got_b = swap(jnp.concatenate([h_b, g_b.reshape(-1, LANES)]), "cols", 2)
    h_a, h_b = h_a + got_a[:cut], h_b + got_b[:cut]
    g_a = ordered(x, g_a, got_a[cut:].reshape(g_a.shape))
    g_b = ordered(y, g_b, got_b[cut:].reshape(g_b.shape))
    gram = jnp.concatenate([jnp.swapaxes(g_a, 0, 1), g_b], axis=2).reshape(-1, LANES)
    own = jnp.stack([jnp.concatenate([h_a, h_b]), gram])
    return whiten(1.0 / total, core, own, swap(own, "cols", 1), basis, new_vectors)


def solution(mesh):
    placed = (P(("rows", "cols"), None), P(("rows", "cols"), None), P(("rows", "cols"), None))
    return jax.shard_map(
        local, mesh=mesh, in_specs=placed, out_specs=P(("rows", "cols"), None), check_vma=False
    )
```

```python
import functools

import jax
import jax.numpy as jnp
from jax import lax
from jax.experimental import pallas as pl
from jax.experimental.pallas import tpu as pltpu
from jax.sharding import PartitionSpec as P

F32 = jnp.float32
BF16 = jnp.bfloat16
LANES = 128
BLOCK = 16
PANEL = 2
CHUNKS = 4
SHARE = 9
LIMIT = pltpu.CompilerParams(vmem_limit_bytes=32 << 20)
VMEM = pltpu.VMEM


def halves(value):
    high = value.astype(BF16)
    return high, (value - high.astype(F32)).astype(BF16)


def thirds(value):
    high = value.astype(BF16)
    rest = value - high.astype(F32)
    middle = rest.astype(BF16)
    return high, middle, (rest - middle.astype(F32)).astype(BF16)


def contract(left, right, left_dim, right_dim):
    return lax.dot_general(
        left, right, (((left_dim,), (right_dim,)), ((), ())), preferred_element_type=F32
    )


def three(left, right, left_dim, right_dim):
    return (
        contract(left[0], right[0], left_dim, right_dim)
        + contract(left[0], right[1], left_dim, right_dim)
        + contract(left[1], right[0], left_dim, right_dim)
    )


def exact(left, right, left_dim, right_dim):
    return lax.dot_general(
        left,
        right,
        (((left_dim,), (right_dim,)), ((), ())),
        precision=lax.Precision.HIGHEST,
        preferred_element_type=F32,
    )


def spread(outs, value, extra):
    lanes = outs[0].shape[2]
    piece = extra.shape[0] // outs[0].shape[0]
    cut = outs[0].shape[1]
    tall = value.shape[0]
    for s in range(outs[0].shape[0]):
        tile = value[:, s * lanes : (s + 1) * lanes]
        outs[0][s, :, :] = tile[:cut]
        outs[1][s, : tall - cut, :] = tile[cut:]
        outs[1][s, tall - cut :, :] = extra[s * piece : (s + 1) * piece]


def products_kernel(first, core_ref, basis_ref, new_ref, jac_ref, *refs):
    if first:
        out_a_ref, out_b_ref, own_ref, vec_ref, obs_ref, sems = refs
    else:
        own_ref, out_a_ref, out_b_ref, vec_ref, obs_ref, sems = refs
    rows, width = basis_ref.shape
    wide = vec_ref.shape[1]
    part = obs_ref.shape[1]
    chunk = rows // CHUNKS
    index = 1 - core_ref[0] if first else core_ref[0]
    lanes = pl.ds(pl.multiple_of(index * part, part), part)

    def copies(k):
        at = pl.ds(k * chunk, chunk)
        return (
            pltpu.make_async_copy(basis_ref.at[at, :], vec_ref.at[at, pl.ds(0, width)], sems.at[k, 0]),
            pltpu.make_async_copy(new_ref.at[at, :], vec_ref.at[at, pl.ds(width, wide - width)], sems.at[k, 1]),
            pltpu.make_async_copy(jac_ref.at[at, lanes], obs_ref.at[at, :], sems.at[k, 2]),
        )

    for k in range(CHUNKS):
        for copy in copies(k):
            copy.start()
    total = None
    for k in range(CHUNKS):
        for copy in copies(k):
            copy.wait()
        at = slice(k * chunk, (k + 1) * chunk)
        value = vec_ref[at, :]
        flipped = halves(value.T)
        sums = [three(flipped, halves(obs_ref[at, :]), 1, 0)]
        if first:
            stacked = halves(value)
            sums += [contract(flipped[0], part, 1, 0) for part in stacked]
        total = sums if total is None else [x + y for x, y in zip(total, sums)]
    if not first:
        spread((out_a_ref, out_b_ref), total[0], own_ref[...])
        return
    prod, near, far = total
    gram = near + far + far.T
    tiles = wide // LANES
    blocks = [gram[i * LANES : (i + 1) * LANES, j * LANES : (j + 1) * LANES] for j in range(tiles) for i in range(j, tiles)]
    half = len(blocks) // 2
    low, high = (jnp.concatenate(blocks[k * half : (k + 1) * half], axis=0) for k in range(2))
    lead = core_ref[0] == 1
    spread((out_a_ref, out_b_ref), prod, jnp.where(lead, low, high))
    own_ref[...] = jnp.where(lead, high, low)


def products(core, basis, new_vectors, jacobian):
    rows, width = basis.shape
    wide = width + new_vectors.shape[1]
    obs = jacobian.shape[1]
    tiles = wide // LANES
    packed = tiles * (tiles + 1) // 2 * LANES // 8
    cut = (wide + packed) * SHARE // 20
    sums = [VMEM((4, size, obs // 8), F32) for size in (cut, wide + packed - cut)]
    own = VMEM((4 * packed, obs // 8), F32)
    inside = pl.BlockSpec(memory_space=VMEM)
    outside = pl.BlockSpec(memory_space=pltpu.HBM)
    scalar = pl.BlockSpec(memory_space=pltpu.SMEM)

    def call(first, *more):
        return pl.pallas_call(
            functools.partial(products_kernel, first),
            in_specs=[scalar, outside, outside, outside] + [inside] * len(more),
            out_specs=[inside] * (3 if first else 2),
            out_shape=[*sums, own] if first else sums,
            scratch_shapes=[
                VMEM((rows, wide), F32),
                VMEM((rows, obs // 2), F32),
                pltpu.SemaphoreType.DMA((CHUNKS, 3)),
            ],
            compiler_params=LIMIT,
        )(core, basis, new_vectors, jacobian, *more)

    *theirs, own = call(True)
    return call(False, own), theirs


def eliminate(parts, tile, first):
    height = parts[0].shape[0]
    row = lax.broadcasted_iota(jnp.int32, (height, LANES), 0)
    lane = lax.broadcasted_iota(jnp.int32, (height, LANES), 1) - first
    cols = [
        jnp.take_along_axis(parts[tile], jnp.full((height, LANES), first + q, jnp.int32), axis=1) for q in range(BLOCK)
    ]
    parts = list(parts)
    parts[tile] = jnp.where((lane >= 0) & (lane < BLOCK), jnp.where(lane == row, 1.0, 0.0), parts[tile])
    head = row[:BLOCK]
    pivots = jnp.ones((BLOCK, LANES), F32)

    def spot(value, index, tall):
        return jnp.broadcast_to(value[index : index + 1, :], (tall, LANES))

    for p in range(0, BLOCK, 2):
        low = (p + 1) // 8 * 8
        a, b, c = spot(cols[p], p, height), spot(cols[p], p + 1, height), spot(cols[p + 1], p + 1, height)
        det = a * c - b * b
        over_det, over_a = 1.0 / det, 1.0 / a
        pivots = jnp.where(head == p, a[:BLOCK], jnp.where(head == p + 1, (det * over_a)[:BLOCK], pivots))
        under = row[low:] > p + 1
        x, y = cols[p][low:], cols[p + 1][low:]
        a, b, c, ratio, over_det = (v[low:] for v in (a, b, c, b * over_a, over_det))
        mult = jnp.where(under, (x * c - y * b) * over_det, 0.0)
        next_mult = jnp.where(under, (y * a - x * b) * over_det, 0.0)

        def cleared(value, first_mult, p=p, low=low, next_mult=next_mult):
            tall = height - low
            new = value[low:] - first_mult * spot(value, p, tall) - next_mult * spot(value, p + 1, tall)
            return jnp.concatenate([value[:low], new], axis=0) if low else new

        for q in range(p + 2, BLOCK):
            cols[q] = cleared(cols[q], mult)
        mult = jnp.where(row[low:] == p + 1, ratio, mult)
        parts = [cleared(value, mult) for value in parts]
    inv = lax.rsqrt(pivots)
    return [value[:BLOCK] * inv for value in parts], [value[BLOCK:] for value in parts]


def factor(m_ref, ready, beside):
    n = m_ref.shape[0]
    tiles = n // LANES
    panel = BLOCK * PANEL
    for phase in range(tiles):
        base = LANES * phase
        last = phase == tiles - 1
        if last:
            ready()

        def step(k, carry, base=base, phase=phase, last=last):
            start = base + k * panel
            if last:
                beside(k)
            mine = pl.ds(pl.multiple_of(start, panel), panel)
            rows = m_ref[mine, :]
            parts = [rows[:, t * LANES : (t + 1) * LANES] for t in range(tiles)]
            blocks = []
            for b in range(PANEL):
                top, parts = eliminate(parts, phase, k * panel + b * BLOCK)
                blocks.append(jnp.concatenate(top, axis=1))
            done = jnp.concatenate(blocks, axis=0)
            lane = lax.broadcasted_iota(jnp.int32, (panel, n), 1) - start
            sub = lax.broadcasted_iota(jnp.int32, (panel, n), 0)
            rest = jnp.where(lane >= panel, done, 0.0)[:, base:]
            done = jnp.where((lane < panel) & (lane > sub), 0.0, done)
            h, m, l = thirds(done)
            hr, mr, lr = thirds(rest)
            right = jnp.concatenate([h, m, h, l, h, m], axis=0)
            left = jnp.concatenate([hr, hr, mr, hr, lr, mr], axis=0)
            update = contract(left, right, 0, 0)
            lanes = lax.broadcasted_iota(jnp.int32, (n - base, n), 1) - start
            keep = (lanes < 0) | (lanes >= panel)
            m_ref[base:, :] = jnp.where(keep, m_ref[base:, :], 0.0) - update
            m_ref[mine, :] = done
            return carry

        lax.fori_loop(0, LANES // panel, step, 0)


def hess_kernel(core_ref, a_ref, got_a_ref, b_ref, got_b_ref, keep_a_ref, keep_b_ref, give_a_ref, give_b_ref, gram_a_ref, gram_b_ref):
    shard = jnp.concatenate([a_ref[...] + got_a_ref[...], b_ref[...] + got_b_ref[...]], axis=0)
    cut = gram_a_ref.shape[0]
    wide = shard.shape[0] - 2 * cut
    tiles = wide // LANES
    hess = exact(shard[:wide], shard[:wide], 1, 1)
    blocks = [
        hess[i * LANES : (i + 1) * LANES, j * LANES : (j + 1) * LANES] for j in range(tiles) for i in range(j, tiles)
    ]
    half = len(blocks) // 2
    first, second = (jnp.concatenate(blocks[k * half : (k + 1) * half], axis=0) for k in range(2))
    lead = core_ref[0] == 1
    keep, give = jnp.where(lead, second, first), jnp.where(lead, first, second)
    middle = keep_a_ref.shape[0]
    keep_a_ref[...], keep_b_ref[...] = keep[:middle], keep[middle:]
    give_a_ref[...], give_b_ref[...] = give[:middle], give[middle:]
    gram_a_ref[...], gram_b_ref[...] = shard[wide : wide + cut], shard[wide + cut :]


def shard_hess(core, wide, a, got_a, b, got_b):
    inside = pl.BlockSpec(memory_space=VMEM)
    tiles = wide // LANES
    part = VMEM((tiles * (tiles + 1) * LANES // 8, LANES), F32)
    gram = VMEM(((a.shape[0] + b.shape[0] - wide) // 2, LANES), F32)
    return pl.pallas_call(
        hess_kernel,
        in_specs=[pl.BlockSpec(memory_space=pltpu.SMEM)] + [inside] * 4,
        out_specs=[inside] * 6,
        out_shape=[part] * 4 + [gram] * 2,
        compiler_params=LIMIT,
    )(core, a, got_a, b, got_b)


def whiten_kernel(scale, lead_ref, own_ref, got_ref, basis_ref, new_ref, out_ref, m_ref, vec_ref, res_ref, mix_ref, sems):
    n = m_ref.shape[0]
    rows, width = basis_ref.shape
    chunk = rows // CHUNKS

    def loads(k):
        at = pl.ds(k * chunk, chunk)
        return (
            pltpu.make_async_copy(basis_ref.at[at, :], vec_ref.at[at, pl.ds(0, width)], sems.at[k, 0]),
            pltpu.make_async_copy(new_ref.at[at, :], vec_ref.at[at, pl.ds(width, n - width)], sems.at[k, 1]),
        )

    for k in range(CHUNKS):
        for copy in loads(k):
            copy.start()
    tiles = n // LANES
    pairs = [(i, j) for j in range(tiles) for i in range(j, tiles)]
    half = len(pairs) // 2
    lead = lead_ref[0] == 1

    def whole(which):
        blocks = {}
        for index, (i, j) in enumerate(pairs):
            rest = index % half * LANES
            at = slice(rest, rest + LANES)
            value = jnp.where(lead == (index >= half), own_ref[which, at, :], got_ref[which, at, :]) * scale
            blocks[i, j] = value
            if i != j:
                blocks[j, i] = value.T
        return jnp.concatenate(
            [jnp.concatenate([blocks[i, j] for j in range(tiles)], axis=1) for i in range(tiles)], axis=0
        )

    hess = whole(0)
    full = whole(1)
    s_vv, s_vw, s_ww = full[:width, :width], full[:width, width:], full[width:, width:]
    second = s_vw - exact(s_vv, s_vw, 1, 0)
    summed = s_vw + second
    moved = second + exact(s_vv, summed, 1, 0)
    corner = s_ww + exact(
        jnp.concatenate([summed, s_vw], axis=0), jnp.concatenate([moved, -summed], axis=0), 0, 0
    )
    r = lax.broadcasted_iota(jnp.int32, (width, width), 0)
    c = lax.broadcasted_iota(jnp.int32, (width, width), 1)
    m_ref[:width, :width] = hess[:width, :width] + jnp.where(r == c, 1.0, 0.0)
    m_ref[:width, width:] = hess[:width, width:] + summed
    m_ref[width:, :width] = hess[width:, :width] + summed.T
    m_ref[width:, width:] = hess[width:, width:] + corner
    lead_cols = n - LANES

    def store(k, late):
        at = pl.ds(pl.multiple_of(k * chunk, chunk), chunk)
        lanes = pl.ds(lead_cols, LANES) if late else pl.ds(0, lead_cols)
        return pltpu.make_async_copy(res_ref.at[at, lanes], out_ref.at[at, lanes], sems.at[k, 2 + late])

    def triangle(low, high):
        r = lax.broadcasted_iota(jnp.int32, (high - low, high), 0) + low
        c = lax.broadcasted_iota(jnp.int32, (high - low, high), 1)
        return halves(jnp.where(r >= c, m_ref[low:high, :high], 0.0).T)

    def ready():
        mix_ref[0], mix_ref[1] = triangle(0, lead_cols)
        for k in range(CHUNKS):
            for copy in loads(k):
                copy.wait()

    def beside(k):
        at = pl.ds(pl.multiple_of(k * chunk, chunk), chunk)
        res_ref[at, :lead_cols] = three(halves(vec_ref[at, :lead_cols]), (mix_ref[0], mix_ref[1]), 1, 0)
        store(k, 0).start()

    factor(m_ref, ready, beside)
    last = triangle(lead_cols, n)
    for k in range(CHUNKS):
        at = slice(k * chunk, (k + 1) * chunk)
        res_ref[at, lead_cols:] = three(halves(vec_ref[at, :]), last, 1, 0)
        store(k, 1).start()
    for k in range(CHUNKS):
        store(k, 0).wait()
        store(k, 1).wait()


def whiten(scale, lead, own, got, basis, new_vectors):
    rows, width = basis.shape
    n = width + new_vectors.shape[1]

    def kernel(*refs):
        whiten_kernel(scale, *refs)

    inside = pl.BlockSpec(memory_space=VMEM)
    outside = pl.BlockSpec(memory_space=pltpu.HBM)
    return pl.pallas_call(
        kernel,
        in_specs=[pl.BlockSpec(memory_space=pltpu.SMEM), inside, inside, outside, outside],
        out_specs=outside,
        out_shape=jax.ShapeDtypeStruct((rows, n), F32),
        scratch_shapes=[
            VMEM((n, n), F32),
            VMEM((rows, n), F32),
            VMEM((rows, n), F32),
            VMEM((2, n - LANES, n - LANES), BF16),
            pltpu.SemaphoreType.DMA((CHUNKS, 4)),
        ],
        compiler_params=LIMIT,
    )(lead, own, got, basis, new_vectors)


def pick(value, index):
    return lax.dynamic_index_in_dim(value, index, 0, keepdims=False)


def ordered(bit, own, other):
    return jnp.stack([jnp.where(bit == 0, own, other), jnp.where(bit == 0, other, own)])


def swap(value, axis, mask):
    size = lax.axis_size(axis)
    return lax.ppermute(value, axis, [(i, i ^ mask) for i in range(size)])


def local(basis, new_vectors, jacobian):
    n_rows, n_cols = lax.axis_size("rows"), lax.axis_size("cols")
    total = basis.shape[0] * n_rows * n_cols
    wide = basis.shape[1] + new_vectors.shape[1]
    at_row, at_col = lax.axis_index("rows"), lax.axis_index("cols")
    core, y, x = (at_col & 1).reshape(1), (at_col >> 1) & 1, at_row & 1
    rest = [("cols", 1 << b) for b in range(2, n_cols.bit_length() - 1)]
    rest += [("rows", m) for m in (2, 6) if m < n_rows]
    rest += [("rows", 1 << b) for b in range(3, n_rows.bit_length() - 1)]

    basis, new_vectors, jacobian = (
        pltpu.with_memory_space_constraint(value, pltpu.HBM) for value in (basis, new_vectors, jacobian)
    )
    mine, theirs = products(core, basis, new_vectors, jacobian)
    a, b = (value.reshape(2, 2, *value.shape[1:]) for value in mine)
    up_a, up_b = (swap(value, "cols", 1).reshape(2, 2, *value.shape[1:]) for value in theirs)

    def across(value, index):
        return lax.dynamic_index_in_dim(value, index, 1, keepdims=False)

    def both(value, up, got, at_y, at_x, index):
        return pick(pick(value, at_y), at_x) + pick(pick(up, at_y), at_x) + pick(got, index)

    got_a = swap(pick(a, 1 - y) + pick(up_a, 1 - y), "cols", 2)
    got_b = swap(across(b, 1 - x) + across(up_b, 1 - x), "rows", 1)
    next_a = swap(both(a, up_a, got_a, y, 1 - x, 1 - x), "rows", 1)
    next_b = swap(both(b, up_b, got_b, 1 - y, x, 1 - y), "cols", 2)
    a, got_a = both(a, up_a, got_a, y, x, x), next_a
    b, got_b = both(b, up_b, got_b, y, x, y), next_b
    for (axis_a, mask_a), (axis_b, mask_b) in zip(rest, rest[::-1]):
        a, b = a + got_a, b + got_b
        got_a = swap(a, axis_a, mask_a)
        got_b = swap(b, axis_b, mask_b)

    keep_a, keep_b, give_a, give_b, g_a, g_b = shard_hess(core, wide, a, got_a, b, got_b)
    h_a, h_b = keep_a + swap(give_a, "cols", 1), keep_b + swap(give_b, "cols", 1)
    cut = h_a.shape[0]
    got_a = swap(jnp.concatenate([h_a, g_a]), "cols", 2)
    got_b = swap(jnp.concatenate([h_b, g_b]), "rows", 1)
    h_a, h_b = h_a + got_a[:cut], h_b + got_b[:cut]
    g_a = ordered(y, g_a, got_a[cut:])
    g_b = ordered(x, g_b, got_b[cut:])
    got_a = swap(jnp.concatenate([h_a, g_a.reshape(-1, LANES)]), "rows", 1)
    got_b = swap(jnp.concatenate([h_b, g_b.reshape(-1, LANES)]), "cols", 2)
    h_a, h_b = h_a + got_a[:cut], h_b + got_b[:cut]
    g_a = ordered(x, g_a, got_a[cut:].reshape(g_a.shape))
    g_b = ordered(y, g_b, got_b[cut:].reshape(g_b.shape))
    gram = jnp.concatenate([jnp.swapaxes(g_a, 0, 1), g_b], axis=2).reshape(-1, LANES)
    own = jnp.stack([jnp.concatenate([h_a, h_b]), gram])
    return whiten(1.0 / total, core, own, swap(own, "cols", 1), basis, new_vectors)


def solution(mesh):
    placed = (P(("rows", "cols"), None), P(("rows", "cols"), None), P(("rows", "cols"), None))
    return jax.shard_map(
        local, mesh=mesh, in_specs=placed, out_specs=P(("rows", "cols"), None), check_vma=False
    )
```
